32 devices in a mesh: row: 8 (over z, x), col: 4 (over y, core).
Axes of the slice: x: 2, y: 2, z: 4, core: 2. Of those that a mesh axis runs over, the one named last changes fastest.
Arguments:
- eigvecs: float32 [16384, 4096], P('row', 'col'), may hold values from -6 to 6
- reflectors: float32 [2, 16384, 256], P(None, ('row', 'col')), may hold values from -0.13258252 to 0.13258252
- tfactors: float32 [2, 256, 256], replicated, may hold values from -1 to 2, as said below
Outputs:
- back: float32 [16384, 4096], P('row', 'col')
The draws below stay inside these ranges and needn't reach their ends.
Inputs may be any that keep to these rules, and one draw needn't show every extreme that they name: Each tfactors[p] is upper triangular; its diagonal lies between 0.3 and 1.9.
All inputs are finite; a program needn't handle non-finite values.
Results may differ from the reference program's by a relative error of at most 0.00014.
Values sent between devices are 32-bit elements; how exact they have to be, the bound alone decides.
A program may use at most 128 MiB of HBM per device.

```python
import jax
import jax.numpy as jnp
from jax import lax

NB = 256
PANELS = 2
N = 16384
K = 4096


def draw_tfactors(key, part):
    first = jax.random.fold_in(key, 11)
    second = jax.random.fold_in(key, 12)
    offdiag = jnp.clip(jax.random.normal(first, (PANELS, NB, NB), jnp.float32), -3.0, 3.0) / jnp.sqrt(jnp.float32(NB))
    diagonal = jax.random.uniform(second, (PANELS, NB), jnp.float32, 0.5, 1.5)
    upper_part = jnp.triu(offdiag, 1)
    eye_mat = jnp.eye(NB, dtype=jnp.float32)
    return (upper_part + eye_mat[None, :, :] * diagonal[:, None, :]).astype(jnp.float32)


def steps_of(rng, shape, cuts, smallest, top_value):
    def one(axis_at, blocks):
        draws = jax.random.uniform(jax.random.fold_in(jax.random.fold_in(rng, 6), axis_at), (blocks,), jnp.float32, smallest / len(cuts), top_value / len(cuts))
        return jnp.repeat(jnp.exp(draws), shape[axis_at] // blocks).reshape((-1,) + (1,) * (len(shape) - axis_at - 1))

    loudness = one(*cuts[0])
    for cut in cuts[1:]:
        loudness = loudness * one(*cut)
    return loudness


def gaussian(rng, dims, spread, bound, cuts=(), kind=jnp.bfloat16):
    loudness = steps_of(rng, dims, cuts, -0.22, 0.18) if cuts else 1.0
    drawn = jax.random.normal(rng, dims, jnp.float32) * spread * loudness
    return jnp.minimum(jnp.maximum(drawn, -bound), bound).astype(kind)


def setup_inputs(seed: int = 0) -> dict:
    seeds = jax.random.split(jax.random.key(seed), 4)
    eigvecs = gaussian(seeds[0], (N, K), 1.0, 6.0, ((0, 8), (1, 4)), jnp.float32)
    reflectors = gaussian(seeds[1], (PANELS, N, NB), ((N * NB) ** -0.25), 0.13258252, ((1, 32),), jnp.float32)
    tfactors = draw_tfactors(jax.random.fold_in(seeds[3], 71), 0)
    return {"eigvecs": eigvecs, "reflectors": reflectors, "tfactors": tfactors}


def product(left, right):
    return jnp.dot(left, right, precision=lax.Precision.HIGHEST, preferred_element_type=jnp.float32)


def reference(eigvecs, reflectors, tfactors):
    current = eigvecs
    for panel_idx in range(PANELS - 1, -1, -1):
        block = reflectors[panel_idx]
        inner_prod = product(block.T, current)
        coeffs = product(tfactors[panel_idx], inner_prod)
        current = current - product(block, coeffs)
    return current
```

```python
import functools

import jax
import jax.numpy as jnp
from jax import lax
from jax.experimental import pallas as pl
from jax.experimental.pallas import tpu as pltpu
from jax.sharding import PartitionSpec as P

F32 = jnp.float32
BF16 = jnp.bfloat16
MESH = pl.DeviceIdType.MESH
TILE = 256


def halves(value):
    high = value.astype(BF16)
    return high, (value - high.astype(F32)).astype(BF16)


def dot3(left, right, contract=((1,), (0,))):
    def one(a, b):
        return lax.dot_general(a, b, (contract, ((), ())), preferred_element_type=F32)

    return one(left[0], right[0]) + (one(left[0], right[1]) + one(left[1], right[0]))


def flip(index, bit):
    return index + (1 - 2 * ((index // bit) % 2)) * bit


def reduce_kernel(rows_n, cols_n, cw, eig, refl, tfac, vhi_out, vlo_out, chi, clo,
                  ebuf, ehi, elo, vbuf, vhi, vlo, g_hi, g_lo, r_hi, r_lo, a_hi, a_lo,
                  load_e, load_v, store_v, v_send, v_recv, rs_send, rs_recv, ag_send, ag_recv):
    row, col = lax.axis_index("row"), lax.axis_index("col")
    panels, part, nb = refl.shape
    block, width = eig.shape
    per = nb // cw
    chunks = panels * per
    row_bits = rows_n.bit_length() - 1
    col_bits = cols_n.bit_length() - 1
    tiles = block // TILE

    def place(k):
        return (1, k) if k < per else (0, k - per)

    def own_load(k):
        panel, part_at = place(k)
        return pltpu.make_async_copy(
            refl.at[panel, :, pl.ds(part_at * cw, cw)], vbuf.at[k, col], load_v.at[k])

    def e_load(t):
        return pltpu.make_async_copy(
            eig.at[pl.ds(t * TILE, TILE), :], ebuf.at[pl.ds(t * TILE, TILE), :], load_e.at[t])

    for k in range(chunks):
        own_load(k).start()
    for t in range(tiles):
        e_load(t).start()

    barrier = pltpu.get_barrier_semaphore()
    for b in range(row_bits):
        pl.semaphore_signal(barrier, inc=1, device_id=(flip(row, 1 << b), col), device_id_type=MESH)
    for b in range(col_bits):
        pl.semaphore_signal(barrier, inc=1, device_id=(row, flip(col, 1 << b)), device_id_type=MESH)
    pl.semaphore_wait(barrier, row_bits + col_bits)

    def rel(r):
        at = col
        for b in range(col_bits):
            if (r >> b) & 1:
                at = flip(at, 1 << b)
        return at

    def v_copy(k, r, b):
        slot = vbuf.at[k, rel(r)]
        return pltpu.make_async_remote_copy(
            src_ref=slot, dst_ref=slot, send_sem=v_send.at[k, r + (1 << b)],
            recv_sem=v_recv.at[k, r + (1 << b)],
            device_id=(row, flip(col, 1 << b)), device_id_type=MESH)

    def v_arrived(k, r):
        low = (r & -r).bit_length() - 1
        slot = vbuf.at[k, rel(r)]
        pltpu.make_async_remote_copy(
            src_ref=slot, dst_ref=slot, send_sem=v_send.at[k, r], recv_sem=v_recv.at[k, r],
            device_id=(row, flip(col, 1 << low)), device_id_type=MESH).wait_recv()

    for k in range(chunks):
        own_load(k).wait()
        for b in reversed(range(col_bits)):
            v_copy(k, 0, b).start()

    for t in range(tiles):
        e_load(t).wait()

    @pl.loop(0, tiles)
    def _(t):
        at = pl.ds(pl.multiple_of(t * TILE, TILE), TILE)
        high, low = halves(ebuf[at, :])
        ehi[at, :] = high
        elo[at, :] = low

    order = sorted(range(1, cols_n), key=lambda r: (-(r & -r), r))

    def buffers(k):
        panel, part_at = place(k)
        g, r, a = (g_hi, r_hi, a_hi) if panel == 1 else (g_lo, r_lo, a_lo)
        return g, r, a, part_at * cw

    def contract(k):
        panel, part_at = place(k)
        for r in order:
            v_arrived(k, r)
            for b in reversed(range((r & -r).bit_length() - 1)):
                v_copy(k, r, b).start()
        lane = panel * nb + part_at * cw
        here = slice(lane, lane + cw)

        for c in range(cols_n):
            high, low = halves(vbuf[k, c])
            vhi[c * part:(c + 1) * part, here] = high
            vlo[c * part:(c + 1) * part, here] = low
        g, _, _, base = buffers(k)
        left = vhi[:, here], vlo[:, here]

        @pl.loop(0, width // TILE)
        def _(n):
            at = pl.ds(pl.multiple_of(n * TILE, TILE), TILE)
            g[base:base + cw, at] = dot3(left, (ehi[:, at], elo[:, at]), ((0,), (0,)))

        if panel == 0:
            upper = slice(nb, 2 * nb)
            g[base:base + cw, width:width + nb] = dot3(left, (vhi[:, upper], vlo[:, upper]), ((0,), (0,)))

    def start_of(level):
        at = 0
        for b in range(level):
            at = at + ((row // (1 << b)) % 2) * (cw >> (b + 1))
        return at

    def rs_copy(k, level):
        g, r, _, base = buffers(k)
        half = cw >> (level + 1)
        bit = (row // (1 << level)) % 2
        src = pl.multiple_of(base + start_of(level) + (1 - bit) * half, 8)
        dst = base + cw - 2 * half
        return pltpu.make_async_remote_copy(
            src_ref=g.at[pl.ds(src, half), :], dst_ref=r.at[pl.ds(dst, half), :],
            send_sem=rs_send.at[k, level], recv_sem=rs_recv.at[k, level],
            device_id=(flip(row, 1 << level), col), device_id_type=MESH)

    def rs_take(k, level):
        g, r, a, base = buffers(k)
        rs_copy(k, level).wait_recv()
        half = cw >> (level + 1)
        keep = pl.ds(pl.multiple_of(base + start_of(level + 1), 8), half)
        came = base + cw - 2 * half
        total = g[keep, :] + r[came:came + half, :]
        if level == row_bits - 1:
            a[keep, :] = total
        else:
            g[keep, :] = total

    def ag_copy(k, level):
        _, _, a, base = buffers(k)
        size = cw >> (level + 1)
        rows = pl.ds(pl.multiple_of(base + start_of(level + 1), 8), size)
        return pltpu.make_async_remote_copy(
            src_ref=a.at[rows, :], dst_ref=a.at[rows, :],
            send_sem=ag_send.at[k, level], recv_sem=ag_recv.at[k, level],
            device_id=(flip(row, 1 << level), col), device_id_type=MESH)

    def ag_take(k, level):
        _, _, a, base = buffers(k)
        size = cw >> (level + 1)
        bit = (row // (1 << level)) % 2
        rows = pl.ds(pl.multiple_of(base + start_of(level) + (1 - bit) * size, 8), size)
        pltpu.make_async_remote_copy(
            src_ref=a.at[rows, :], dst_ref=a.at[rows, :],
            send_sem=ag_send.at[k, level], recv_sem=ag_recv.at[k, level],
            device_id=(flip(row, 1 << level), col), device_id_type=MESH).wait_recv()

    def stage(k, s):
        if s == 0:
            contract(k)
            rs_copy(k, 0).start()
        elif s < row_bits:
            rs_take(k, s - 1)
            rs_copy(k, s).start()
        elif s == row_bits:
            rs_take(k, s - 1)
            ag_copy(k, row_bits - 1).start()
        else:
            level = 2 * row_bits - s
            ag_take(k, level)
            if level:
                ag_copy(k, level - 1).start()

    stages = 2 * row_bits + 1
    for slot in range(chunks + stages - 1):
        for k in range(chunks):
            if 0 <= slot - k < stages:
                stage(k, slot - k)
        if slot == chunks - 1:
            keep_hi = pltpu.make_async_copy(vhi, vhi_out, store_v.at[0])
            keep_lo = pltpu.make_async_copy(vlo, vlo_out, store_v.at[1])
            keep_hi.start()
            keep_lo.start()

    upper_t, lower_t = halves(tfac[1]), halves(tfac[0])
    gram = halves(a_lo[:, width:width + nb])

    @pl.loop(0, width // TILE)
    def _(n):
        at = pl.ds(pl.multiple_of(n * TILE, TILE), TILE)
        high = halves(dot3(upper_t, halves(a_hi[:, at])))
        low = halves(dot3(lower_t, halves(a_lo[:, at] - dot3(gram, high))))
        chi[0:nb, at] = low[0]
        clo[0:nb, at] = low[1]
        chi[nb:2 * nb, at] = high[0]
        clo[nb:2 * nb, at] = high[1]

    for k in range(chunks):
        for r in range(cols_n):
            low = (r & -r).bit_length() - 1 if r else col_bits
            for b in range(low):
                v_copy(k, r, b).wait_send()
        for level in range(row_bits):
            rs_copy(k, level).wait_send()
            ag_copy(k, level).wait_send()
    keep_hi.wait()
    keep_lo.wait()


def update_kernel(eig, vhi, vlo, chi, clo, out):
    out[...] = eig[...] - dot3((vhi[...], vlo[...]), (chi[...], clo[...]))


def local(rows_n, cols_n, eigvecs, reflectors, tfactors):
    panels, part, nb = reflectors.shape
    block, width = eigvecs.shape
    cw = max(128, 8 * rows_n)
    chunks = panels * nb // cw
    row_bits = rows_n.bit_length() - 1
    total = panels * nb
    anywhere = pl.BlockSpec(memory_space=pl.ANY)
    vmem = pl.BlockSpec(memory_space=pltpu.VMEM)
    dma = pltpu.SemaphoreType.DMA
    pair = lambda: [pltpu.VMEM((nb, width), F32), pltpu.VMEM((nb, width + nb), F32)]
    vhi, vlo, chi, clo = pl.pallas_call(
        functools.partial(reduce_kernel, rows_n, cols_n, cw),
        out_shape=[jax.ShapeDtypeStruct((block, total), BF16)] * 2
        + [jax.ShapeDtypeStruct((total, width), BF16)] * 2,
        in_specs=[anywhere, anywhere, vmem],
        out_specs=[anywhere, anywhere, vmem, vmem],
        scratch_shapes=[
            pltpu.VMEM((block, width), F32),
            pltpu.VMEM((block, width), BF16),
            pltpu.VMEM((block, width), BF16),
            pltpu.VMEM((chunks, cols_n, part, cw), F32),
            pltpu.VMEM((block, total), BF16),
            pltpu.VMEM((block, total), BF16),
            *pair(), *pair(), *pair(),
            dma((block // TILE,)), dma((chunks,)), dma((2,)),
            dma((chunks, cols_n)), dma((chunks, cols_n)),
            dma((chunks, row_bits)), dma((chunks, row_bits)),
            dma((chunks, row_bits)), dma((chunks, row_bits)),
        ],
        compiler_params=pltpu.CompilerParams(
            collective_id=0, has_side_effects=True, vmem_limit_bytes=60 * 1024 * 1024),
    )(eigvecs, reflectors, tfactors)
    rows = 256
    return pl.pallas_call(
        update_kernel,
        grid=(block // rows,),
        out_shape=jax.ShapeDtypeStruct((block, width), F32),
        in_specs=[
            pl.BlockSpec((rows, width), lambda i: (i, 0)),
            pl.BlockSpec((rows, total), lambda i: (i, 0)),
            pl.BlockSpec((rows, total), lambda i: (i, 0)),
            pl.BlockSpec((total, width), lambda i: (0, 0)),
            pl.BlockSpec((total, width), lambda i: (0, 0)),
        ],
        out_specs=pl.BlockSpec((rows, width), lambda i: (i, 0)),
    )(eigvecs, vhi, vlo, chi, clo)


def solution(mesh):
    return jax.shard_map(
        functools.partial(local, mesh.shape["row"], mesh.shape["col"]),
        mesh=mesh,
        in_specs=(P("row", "col"), P(None, ("row", "col"), None), P()),
        out_specs=P("row", "col"),
        check_vma=False,
    )
```

```python
import functools

import jax
import jax.numpy as jnp
from jax import lax
from jax.experimental import pallas as pl
from jax.experimental.pallas import tpu as pltpu
from jax.sharding import PartitionSpec as P

F32 = jnp.float32
BF16 = jnp.bfloat16
MESH = pl.DeviceIdType.MESH
TILE = 256


def halves(value):
    high = value.astype(BF16)
    return high, (value - high.astype(F32)).astype(BF16)


def dot3(left, right, contract=((1,), (0,))):
    def one(a, b):
        return lax.dot_general(a, b, (contract, ((), ())), preferred_element_type=F32)

    return one(left[0], right[0]) + (one(left[0], right[1]) + one(left[1], right[0]))


def flip(index, bit):
    return index + (1 - 2 * ((index // bit) % 2)) * bit


def reduce_kernel(rows_n, cols_n, cw, eig, refl, tfac, vhi_out, vlo_out, chi, clo,
                  ebuf, ehi, elo, vbuf, vhi, vlo, g_hi, g_lo, r_hi, r_lo, a_hi, a_lo,
                  load_e, load_v, store_v, v_send, v_recv, rs_send, rs_recv, ag_send, ag_recv):
    row, col = lax.axis_index("row"), lax.axis_index("col")
    panels, part, nb = refl.shape
    block, width = eig.shape
    per = nb // cw
    chunks = panels * per
    row_bits = rows_n.bit_length() - 1
    col_bits = cols_n.bit_length() - 1
    tiles = block // TILE

    def place(k):
        return (1, k) if k < per else (0, k - per)

    def own_load(k):
        panel, part_at = place(k)
        return pltpu.make_async_copy(
            refl.at[panel, :, pl.ds(part_at * cw, cw)], vbuf.at[k, col], load_v.at[k])

    def e_load(t):
        return pltpu.make_async_copy(
            eig.at[pl.ds(t * TILE, TILE), :], ebuf.at[pl.ds(t * TILE, TILE), :], load_e.at[t])

    for k in range(chunks):
        own_load(k).start()
    for t in range(tiles):
        e_load(t).start()

    barrier = pltpu.get_barrier_semaphore()
    for b in range(row_bits):
        pl.semaphore_signal(barrier, inc=1, device_id=(flip(row, 1 << b), col), device_id_type=MESH)
    for b in range(col_bits):
        pl.semaphore_signal(barrier, inc=1, device_id=(row, flip(col, 1 << b)), device_id_type=MESH)
    pl.semaphore_wait(barrier, row_bits + col_bits)

    def rel(r):
        at = col
        for b in range(col_bits):
            if (r >> b) & 1:
                at = flip(at, 1 << b)
        return at

    def v_copy(k, r, b):
        slot = vbuf.at[k, rel(r)]
        return pltpu.make_async_remote_copy(
            src_ref=slot, dst_ref=slot, send_sem=v_send.at[k, r + (1 << b)],
            recv_sem=v_recv.at[k, r + (1 << b)],
            device_id=(row, flip(col, 1 << b)), device_id_type=MESH)

    def v_arrived(k, r):
        low = (r & -r).bit_length() - 1
        slot = vbuf.at[k, rel(r)]
        pltpu.make_async_remote_copy(
            src_ref=slot, dst_ref=slot, send_sem=v_send.at[k, r], recv_sem=v_recv.at[k, r],
            device_id=(row, flip(col, 1 << low)), device_id_type=MESH).wait_recv()

    for k in range(chunks):
        own_load(k).wait()
        for b in reversed(range(col_bits)):
            v_copy(k, 0, b).start()

    for t in range(tiles):
        e_load(t).wait()

    @pl.loop(0, tiles)
    def _(t):
        at = pl.ds(pl.multiple_of(t * TILE, TILE), TILE)
        high, low = halves(ebuf[at, :])
        ehi[at, :] = high
        elo[at, :] = low

    order = sorted(range(1, cols_n), key=lambda r: (-(r & -r), r))

    def buffers(k):
        panel, part_at = place(k)
        g, r, a = (g_hi, r_hi, a_hi) if panel == 1 else (g_lo, r_lo, a_lo)
        return g, r, a, part_at * cw

    relayed = [r for r in order if r % 2 == 0]
    direct = [r for r in order if r % 2]

    def relay(k):
        for r in relayed:
            v_arrived(k, r)
            for b in reversed(range((r & -r).bit_length() - 1)):
                v_copy(k, r, b).start()

    def contract(k):
        panel, part_at = place(k)
        for r in direct:
            v_arrived(k, r)
        lane = panel * nb + part_at * cw
        here = slice(lane, lane + cw)

        for c in range(cols_n):
            high, low = halves(vbuf[k, c])
            vhi[c * part:(c + 1) * part, here] = high
            vlo[c * part:(c + 1) * part, here] = low
        g, _, _, base = buffers(k)
        left = vhi[:, here], vlo[:, here]
        both = jnp.concatenate(left, axis=1)

        @pl.loop(0, width // TILE)
        def _(n):
            at = pl.ds(pl.multiple_of(n * TILE, TILE), TILE)
            first = lax.dot_general(both, ehi[:, at], (((0,), (0,)), ((), ())), preferred_element_type=F32)
            second = lax.dot_general(left[0], elo[:, at], (((0,), (0,)), ((), ())), preferred_element_type=F32)
            g[base:base + cw, at] = first[:cw] + (first[cw:] + second)

        if panel == 0:
            upper = slice(nb, 2 * nb)
            g[base:base + cw, width:width + nb] = dot3(left, (vhi[:, upper], vlo[:, upper]), ((0,), (0,)))

    upward = list(range(row_bits))
    orders = (upward, upward[1:] + upward[:1])

    def bit_of(p, level):
        return (row // (1 << orders[p][level])) % 2

    def start_of(p, level):
        at = 0
        for b in range(level):
            at = at + bit_of(p, b) * (cw >> (b + 1))
        return at

    def lanes(buffer, p):
        middle = width // 2
        return slice(0, middle) if p == 0 else slice(middle, buffer.shape[1])

    def rs_copy(k, p, level):
        g, r, _, base = buffers(k)
        half = cw >> (level + 1)
        src = pl.multiple_of(base + start_of(p, level) + (1 - bit_of(p, level)) * half, 8)
        dst = base + cw - 2 * half
        here = lanes(g, p)
        return pltpu.make_async_remote_copy(
            src_ref=g.at[pl.ds(src, half), here], dst_ref=r.at[pl.ds(dst, half), here],
            send_sem=rs_send.at[k, p, level], recv_sem=rs_recv.at[k, p, level],
            device_id=(flip(row, 1 << orders[p][level]), col), device_id_type=MESH)

    def rs_take(k, p, level):
        g, r, a, base = buffers(k)
        rs_copy(k, p, level).wait_recv()
        half = cw >> (level + 1)
        keep = pl.ds(pl.multiple_of(base + start_of(p, level + 1), 8), half)
        came = base + cw - 2 * half
        here = lanes(g, p)
        total = g[keep, here] + r[came:came + half, here]
        if level == row_bits - 1:
            a[keep, here] = total
        else:
            g[keep, here] = total

    def ag_at(k, p, level, mine):
        _, _, a, base = buffers(k)
        size = cw >> (level + 1)
        bit = bit_of(p, level) if mine else 1 - bit_of(p, level)
        rows = pl.ds(pl.multiple_of(base + start_of(p, level) + bit * size, 8), size)
        slot = a.at[rows, lanes(a, p)]
        return pltpu.make_async_remote_copy(
            src_ref=slot, dst_ref=slot,
            send_sem=ag_send.at[k, p, level], recv_sem=ag_recv.at[k, p, level],
            device_id=(flip(row, 1 << orders[p][level]), col), device_id_type=MESH)

    def stage(k, s):
        if s == 0:
            contract(k)
        for p in range(2):
            if s == 0:
                rs_copy(k, p, 0).start()
            elif s < row_bits:
                rs_take(k, p, s - 1)
                rs_copy(k, p, s).start()
            elif s == row_bits:
                rs_take(k, p, s - 1)
                ag_at(k, p, row_bits - 1, True).start()
            else:
                level = 2 * row_bits - s
                ag_at(k, p, level, False).wait_recv()
                if level:
                    ag_at(k, p, level - 1, True).start()

    stages = 2 * row_bits + 1
    relay(0)
    for slot in range(chunks - 1 + stages):
        for k in reversed(range(chunks)):
            if 0 <= slot - k < stages:
                stage(k, slot - k)
        if slot + 1 < chunks:
            relay(slot + 1)
        if slot == chunks - 1:
            keep_hi = pltpu.make_async_copy(vhi, vhi_out, store_v.at[0])
            keep_lo = pltpu.make_async_copy(vlo, vlo_out, store_v.at[1])
            keep_hi.start()
            keep_lo.start()

    upper_t, lower_t = halves(tfac[1]), halves(tfac[0])
    gram = halves(a_lo[:, width:width + nb])

    @pl.loop(0, width // TILE)
    def _(n):
        at = pl.ds(pl.multiple_of(n * TILE, TILE), TILE)
        high = halves(dot3(upper_t, halves(a_hi[:, at])))
        low = halves(dot3(lower_t, halves(a_lo[:, at] - dot3(gram, high))))
        chi[0:nb, at] = low[0]
        clo[0:nb, at] = low[1]
        chi[nb:2 * nb, at] = high[0]
        clo[nb:2 * nb, at] = high[1]

    for k in range(chunks):
        for r in range(cols_n):
            low = (r & -r).bit_length() - 1 if r else col_bits
            for b in range(low):
                v_copy(k, r, b).wait_send()
        for p in range(2):
            for level in range(row_bits):
                rs_copy(k, p, level).wait_send()
                ag_at(k, p, level, True).wait_send()
    keep_hi.wait()
    keep_lo.wait()


def update_kernel(eig, vhi, vlo, chi, clo, out):
    out[...] = eig[...] - dot3((vhi[...], vlo[...]), (chi[...], clo[...]))


def local(rows_n, cols_n, eigvecs, reflectors, tfactors):
    panels, part, nb = reflectors.shape
    block, width = eigvecs.shape
    cw = max(128, 8 * rows_n)
    chunks = panels * nb // cw
    row_bits = rows_n.bit_length() - 1
    total = panels * nb
    anywhere = pl.BlockSpec(memory_space=pl.ANY)
    vmem = pl.BlockSpec(memory_space=pltpu.VMEM)
    dma = pltpu.SemaphoreType.DMA
    pair = lambda: [pltpu.VMEM((nb, width), F32), pltpu.VMEM((nb, width + nb), F32)]
    vhi, vlo, chi, clo = pl.pallas_call(
        functools.partial(reduce_kernel, rows_n, cols_n, cw),
        out_shape=[jax.ShapeDtypeStruct((block, total), BF16)] * 2
        + [jax.ShapeDtypeStruct((total, width), BF16)] * 2,
        in_specs=[anywhere, anywhere, vmem],
        out_specs=[anywhere, anywhere, vmem, vmem],
        scratch_shapes=[
            pltpu.VMEM((block, width), F32),
            pltpu.VMEM((block, width), BF16),
            pltpu.VMEM((block, width), BF16),
            pltpu.VMEM((chunks, cols_n, part, cw), F32),
            pltpu.VMEM((block, total), BF16),
            pltpu.VMEM((block, total), BF16),
            *pair(), *pair(), *pair(),
            dma((block // TILE,)), dma((chunks,)), dma((2,)),
            dma((chunks, cols_n)), dma((chunks, cols_n)),
            dma((chunks, 2, row_bits)), dma((chunks, 2, row_bits)),
            dma((chunks, 2, row_bits)), dma((chunks, 2, row_bits)),
        ],
        compiler_params=pltpu.CompilerParams(
            collective_id=0, has_side_effects=True, vmem_limit_bytes=60 * 1024 * 1024),
    )(eigvecs, reflectors, tfactors)
    rows = 512
    return pl.pallas_call(
        update_kernel,
        grid=(block // rows,),
        out_shape=jax.ShapeDtypeStruct((block, width), F32),
        in_specs=[
            pl.BlockSpec((rows, width), lambda i: (i, 0)),
            pl.BlockSpec((rows, total), lambda i: (i, 0)),
            pl.BlockSpec((rows, total), lambda i: (i, 0)),
            pl.BlockSpec((total, width), lambda i: (0, 0)),
            pl.BlockSpec((total, width), lambda i: (0, 0)),
        ],
        out_specs=pl.BlockSpec((rows, width), lambda i: (i, 0)),
    )(eigvecs, vhi, vlo, chi, clo)


def solution(mesh):
    return jax.shard_map(
        functools.partial(local, mesh.shape["row"], mesh.shape["col"]),
        mesh=mesh,
        in_specs=(P("row", "col"), P(None, ("row", "col"), None), P()),
        out_specs=P("row", "col"),
        check_vma=False,
    )
```
